32 devices in a mesh: seq: 8 (over z, x), head: 4 (over y, core).
Axes of the slice: x: 2, y: 2, z: 4, core: 2. Of those that a mesh axis runs over, the one named last changes fastest.
Arguments:
- queries: bfloat16 [8, 64, 128], P('seq', 'head'), may hold values from -90 to 90
- keys: bfloat16 [8, 8, 4096, 128], P(None, 'head', 'seq'), may hold values from -4 to 4
- values: bfloat16 [8, 8, 4096, 128], P(None, 'head', 'seq'), may hold values from -6 to 6
- old_scores: float32 [8, 8, 4096], P(None, 'head', 'seq'), may hold values from 0 to 4
- lengths: int32 [8], replicated, may hold values from 1024 to 4096
- valid_counts: int32 [8, 32], P(None, 'seq'), may hold values from 1 to 128
Outputs:
- attended: bfloat16 [8, 64, 128], P('seq', 'head')
- heavy_scores: float32 [8, 8, 4096], P(None, 'head', 'seq')
The draws below stay inside these ranges and needn't reach their ends.
Inputs may be any that keep to these rules, and one draw needn't show every extreme that they name: `lengths`: slot c of a sequence is cached when c is below its length. `valid_counts`: in block k of a sequence, the slots k * 128 + j with j below the count are live and the others are evicted.
All inputs are finite; a program needn't handle non-finite values.
Results may differ from the reference program's by a relative error of at most 0.0075.
Values may be sent and summed in bfloat16 or wider, within the bound.
A program may use at most 64 MiB of HBM per device.

```python
import jax
import jax.numpy as jnp
from jax import lax

QH = 64
KVH = 8
HD = 128
BLK = 128
SEQS = 8
CTX = 4096
NBLK = 32


def anchor_rows(key):
    return jnp.clip(jax.random.normal(jax.random.fold_in(key, 13), (SEQS, KVH, HD), jnp.float32), -4.0, 4.0)


def draw_keys(key, part):
    bulk = jnp.clip(jax.random.normal(jax.random.fold_in(key, 12), (SEQS, KVH, CTX, HD), jnp.float32), -4.0, 4.0)
    anchor = anchor_rows(key)
    bulk = bulk.at[:, :, 0, :].set(anchor)
    return bulk.astype(jnp.bfloat16)


def draw_queries(key, part):
    bulk = jnp.clip(jax.random.normal(jax.random.fold_in(key, 11), (SEQS, QH, HD), jnp.float32), -4.0, 4.0)
    log_scale = jax.random.uniform(jax.random.fold_in(key, 14), (SEQS, QH, 1), jnp.float32, 0.0, jnp.log(4.0))
    bulk = bulk * jnp.exp(log_scale)
    return bulk.astype(jnp.bfloat16)


def touch_ends(values, own_key, low, top_value):
    index_at = [jax.random.randint(jax.random.fold_in(own_key, axis), (), 0, length) for axis, length in enumerate(values.shape)]
    widest = values.shape.index(max(values.shape))
    next_to = index_at[:widest] + [(index_at[widest] + 1) % values.shape[widest]] + index_at[widest + 1:]
    return values.at[tuple(index_at)].set(low).at[tuple(next_to)].set(top_value)


def level_of(stream_key, extent, pieces, least, high):
    gain, own = 1.0, jax.random.fold_in(stream_key, 6)
    for dim, blocks in pieces:
        heights = jnp.exp(jax.random.uniform(jax.random.fold_in(own, dim), (blocks,), jnp.float32, least / len(pieces), high / len(pieces)))
        gain = gain * jnp.repeat(heights, extent[dim] // blocks).reshape([-1 if axis == dim else 1 for axis in range(len(extent))])
    return gain


def centred(rng, shape, scale, limit, shards=(), held_as=jnp.bfloat16):
    result = scale * jax.random.normal(rng, shape, jnp.float32)
    if shards:
        result = result * level_of(rng, shape, shards, -0.22, 0.18)
    return jnp.clip(result, -limit, limit).astype(held_as)


def setup_inputs(seed: int = 0) -> dict:
    splits = jax.random.split(jax.random.key(seed), 7)
    queries = draw_queries(jax.random.fold_in(splits[6], 71), 0)
    keys = draw_keys(jax.random.fold_in(splits[6], 71), 0)
    values = centred(splits[2], (SEQS, KVH, CTX, HD), 1.0, 6.0, ((1, 4), (2, 8)))
    old_scores = jnp.clip(4.0 * jax.random.uniform(splits[3], (SEQS, KVH, CTX), jnp.float32) ** level_of(splits[3], (SEQS, KVH, CTX), ((1, 4), (2, 8)), -0.2, 0.2), 0.0, 4.0)
    lengths = touch_ends(jax.random.randint(splits[4], (SEQS,), CTX // 4, CTX + 1), jax.random.fold_in(splits[4], 1), CTX // 4, CTX).astype(jnp.int32)
    valid_counts = touch_ends(jax.random.randint(splits[5], (SEQS, NBLK), 1, BLK + 1), jax.random.fold_in(splits[5], 1), 1, BLK).astype(jnp.int32)
    return dict(queries=queries, keys=keys, values=values, old_scores=old_scores, lengths=lengths, valid_counts=valid_counts)


def one_sequence(sequence_item):
    query_rows, key_rows, value_rows, old_rows, length, counts = sequence_item
    group_size = QH // KVH
    grouped = query_rows.astype(jnp.float32).reshape(KVH, group_size, HD)
    scores = jnp.einsum("hgd,hcd->hgc", grouped, key_rows.astype(jnp.float32)) * (HD ** -0.5)
    position = jnp.arange(CTX, dtype=jnp.int32)
    live_mask = (position < length) & ((position % BLK) < jnp.repeat(counts, BLK))
    masked = jnp.where(live_mask[None, None, :], scores, -jnp.inf)
    row_top = jnp.max(masked, axis=2, keepdims=True)
    exponent = jnp.exp(masked - row_top)
    row_total = jnp.sum(exponent, axis=2, keepdims=True)
    weights = lax.optimization_barrier(exponent.astype(jnp.bfloat16))
    mixed_rows = jnp.einsum("hgc,hcd->hgd", weights.astype(jnp.float32), value_rows.astype(jnp.float32))
    attended = (mixed_rows / row_total).astype(jnp.bfloat16).reshape(QH, HD)
    heavy_rows = old_rows + jnp.sum(exponent / row_total, axis=1)
    return attended, heavy_rows


def reference(queries, keys, values, old_scores, lengths, valid_counts):
    attended, heavy_scores = lax.map(one_sequence, (queries, keys, values, old_scores, lengths, valid_counts))
    return attended, heavy_scores
```

```python
import functools

import jax
import jax.numpy as jnp
from jax import lax
from jax.experimental import pallas as pl
from jax.experimental.pallas import tpu as pltpu
from jax.sharding import PartitionSpec as P

BLK = 128
LANES = 128
NEG = -1e30
MESH = pl.DeviceIdType.MESH


def flipped(me, code):
    out = me
    bit = 1
    while bit <= code:
        if code & bit:
            out = out + bit * (1 - 2 * ((me // bit) % 2))
        bit *= 2
    return out


def kernel(n, kv, group, ctx, q_hbm, k_hbm, v_hbm, old_hbm, len_hbm, cnt_hbm,
           att_ref, heavy_ref,
           q_all, k_all, v_all, old_all, len_s, cnt_s, prob, part_out, part_in, stat,
           q_dma, k_dma, v_dma, misc_dma, q_send, q_recv, p_send, p_recv, s_send, s_recv):
    me = lax.axis_index("seq")
    rows = kv * group
    blocks = ctx // BLK
    stat_rows = (n * rows) // LANES
    hd = q_all.shape[-1]
    scale = hd ** -0.5
    seqs = [flipped(me, c) for c in range(n)]

    barrier = pltpu.get_barrier_semaphore()
    for c in range(1, n):
        pl.semaphore_signal(barrier, inc=1, device_id={"seq": seqs[c]}, device_id_type=MESH)

    q_copy = pltpu.make_async_copy(q_hbm.at[0], q_all.at[0], q_dma)
    q_copy.start()
    len_copy = pltpu.make_async_copy(len_hbm, len_s, misc_dma.at[0])
    len_copy.start()
    cnt_copy = pltpu.make_async_copy(cnt_hbm, cnt_s, misc_dma.at[1])
    cnt_copy.start()
    k_copies = [pltpu.make_async_copy(k_hbm.at[seqs[c]], k_all.at[c], k_dma.at[c]) for c in range(n)]
    v_copies = [pltpu.make_async_copy(v_hbm.at[seqs[c]], v_all.at[c], v_dma.at[c]) for c in range(n)]
    for c in range(n):
        k_copies[c].start()
        v_copies[c].start()
    old_copy = pltpu.make_async_copy(old_hbm, old_all, misc_dma.at[2])
    old_copy.start()

    q_copy.wait()
    pl.semaphore_wait(barrier, n - 1)

    def to_peer(src, dst, send_sem, recv_sem, c):
        return pltpu.make_async_remote_copy(
            src_ref=src, dst_ref=dst, send_sem=send_sem, recv_sem=recv_sem,
            device_id={"seq": seqs[c]}, device_id_type=MESH)

    q_sends = [to_peer(q_all.at[0], q_all.at[c], q_send.at[c], q_recv.at[c], c) for c in range(1, n)]
    for copy in reversed(q_sends):
        copy.start()

    lane = lax.broadcasted_iota(jnp.int32, (group, LANES), 1)
    sub = lax.broadcasted_iota(jnp.int32, (group, LANES), 0)
    lane_pair = lane // group
    per_row = LANES // group
    tops = [jnp.zeros((group, LANES), jnp.float32) for _ in range(stat_rows)]
    totals = [jnp.zeros((group, LANES), jnp.float32) for _ in range(stat_rows)]

    len_copy.wait()
    cnt_copy.wait()
    p_sends = []
    half = max(n // 2, 1)
    steps = [list(range(0, 1)), list(range(1, half)), list(range(half, n))]
    for codes in steps:
        for c in codes:
            if c:
                q_sends[c - 1].wait_recv()
            k_copies[c].wait()
            v_copies[c].wait()
        raw = {}
        for c in codes:
            for g in range(kv):
                full = lax.dot_general(q_all[c], k_all[c, g], (((1,), (1,)), ((), ())),
                                       preferred_element_type=jnp.float32)
                raw[c, g] = full[g * group:(g + 1) * group] * scale
        tight = {}
        for c in codes:
            b = seqs[c]
            seen = len_s[b] - me * ctx
            limits = [jnp.minimum(cnt_s[k, b], seen - k * BLK) for k in range(blocks)]
            for g in range(kv):
                masked = jnp.concatenate(
                    [jnp.where(lane < limits[k], raw[c, g][:, k * BLK:(k + 1) * BLK], NEG)
                     for k in range(blocks)], axis=1)
                top = jnp.max(masked, axis=1, keepdims=True)
                p = jnp.exp(masked - top)
                prob[c, g] = p
                total = jnp.sum(p, axis=1, keepdims=True)
                tight[c, g] = p
                pair = b * kv + g
                for r in range(stat_rows):
                    here = lane_pair == pair - r * per_row
                    tops[r] = jnp.where(here, top, tops[r])
                    totals[r] = jnp.where(here, total, totals[r])
        for c in codes:
            wide = jnp.concatenate([tight[c, g] for g in range(kv)], axis=0).astype(jnp.bfloat16)
            mixed = jnp.concatenate(
                [jnp.dot(wide, v_all[c, g], preferred_element_type=jnp.float32)[g * group:(g + 1) * group]
                 for g in range(kv)], axis=0)
            if c:
                part_out[c] = mixed
            else:
                part_in[0] = mixed
        if codes is steps[-1]:
            diag = (lane % group) == sub
            for r in range(stat_rows):
                stat[0, r:r + 1, :] = jnp.sum(jnp.where(diag, tops[r], 0.0), axis=0, keepdims=True)
                stat[0, stat_rows + r:stat_rows + r + 1, :] = jnp.sum(
                    jnp.where(diag, totals[r], 0.0), axis=0, keepdims=True)
        for c in codes:
            if c:
                copy = to_peer(part_out.at[c], part_in.at[c], p_send.at[c], p_recv.at[c], c)
                copy.start()
                p_sends.append(copy)

    s_sends = [to_peer(stat.at[0], stat.at[c], s_send.at[c], s_recv.at[c], c) for c in range(1, n)]
    for copy in reversed(s_sends):
        copy.start()
    old_copy.wait()
    for copy in s_sends:
        copy.wait_recv()

    fac = [[None] * stat_rows for _ in range(n)]
    for r in range(stat_rows):
        top_rows = [jnp.broadcast_to(stat[c, r:r + 1, :], (group, LANES)) for c in range(n)]
        tot_rows = [jnp.broadcast_to(stat[c, stat_rows + r:stat_rows + r + 1, :], (group, LANES)) for c in range(n)]
        best = functools.reduce(jnp.maximum, top_rows)
        scaled = [jnp.exp(t - best) for t in top_rows]
        whole = functools.reduce(jnp.add, [f * t for f, t in zip(scaled, tot_rows)])
        for c in range(n):
            fac[c][r] = scaled[c] / whole

    def column(row_list, pair):
        kept = [jnp.where(lane == pair * group - r * LANES + sub, row_list[r], 0.0)
                for r in range(stat_rows)]
        return jnp.sum(functools.reduce(jnp.add, kept), axis=1, keepdims=True)

    for c in range(n):
        b = seqs[c]
        for g in range(kv):
            share = column(fac[0], b * kv + g)
            add = jnp.sum(prob[c, g] * share, axis=0, keepdims=True)
            heavy_ref[b, g:g + 1, :] = old_all[b, g:g + 1, :] + add

    shares = [jnp.concatenate([column(fac[c], me * kv + g) for g in range(kv)], axis=0) for c in range(n)]
    for copy in p_sends:
        copy.wait_recv()
    att_ref[0] = functools.reduce(
        jnp.add, [shares[c] * part_in[c] for c in range(n)]).astype(jnp.bfloat16)
    for copy in q_sends + p_sends + s_sends:
        copy.wait_send()


def on_device(n, queries, keys, values, old_scores, lengths, valid_counts):
    own, rows, hd = queries.shape
    _, kv, ctx, _ = keys.shape
    group = rows // kv
    assert own == 1 and n & (n - 1) == 0 and (n * rows) % LANES == 0
    counts = valid_counts.T
    stat_rows = (n * rows) // LANES
    anywhere = pl.BlockSpec(memory_space=pl.ANY)
    vmem = pl.BlockSpec(memory_space=pltpu.VMEM)
    dma = pltpu.SemaphoreType.DMA
    return pl.pallas_call(
        functools.partial(kernel, n, kv, group, ctx),
        out_shape=(jax.ShapeDtypeStruct((own, rows, hd), jnp.bfloat16),
                   jax.ShapeDtypeStruct(old_scores.shape, jnp.float32)),
        in_specs=[anywhere] * 6,
        out_specs=(vmem, vmem),
        scratch_shapes=[
            pltpu.VMEM((n, rows, hd), jnp.bfloat16),
            pltpu.VMEM((n, kv, ctx, hd), jnp.bfloat16),
            pltpu.VMEM((n, kv, ctx, hd), jnp.bfloat16),
            pltpu.VMEM(old_scores.shape, jnp.float32),
            pltpu.SMEM(lengths.shape, jnp.int32),
            pltpu.SMEM(counts.shape, jnp.int32),
            pltpu.VMEM((n, kv, group, ctx), jnp.float32),
            pltpu.VMEM((n, rows, hd), jnp.float32),
            pltpu.VMEM((n, rows, hd), jnp.float32),
            pltpu.VMEM((n, 2 * stat_rows, LANES), jnp.float32),
            dma, dma((n,)), dma((n,)), dma((3,)),
            dma((n,)), dma((n,)), dma((n,)), dma((n,)), dma((n,)), dma((n,)),
        ],
        compiler_params=pltpu.CompilerParams(collective_id=0, has_side_effects=True),
    )(queries, keys, values, old_scores, lengths, counts)


def solution(mesh):
    return jax.shard_map(
        functools.partial(on_device, mesh.shape["seq"]),
        mesh=mesh,
        in_specs=(
            P("seq", "head", None),
            P(None, "head", "seq", None),
            P(None, "head", "seq", None),
            P(None, "head", "seq"),
            P(),
            P(None, "seq"),
        ),
        out_specs=(P("seq", "head", None), P(None, "head", "seq")),
        check_vma=False,
    )
```

```python
import functools

import jax
import jax.numpy as jnp
from jax import lax
from jax.experimental import pallas as pl
from jax.experimental.pallas import tpu as pltpu
from jax.sharding import PartitionSpec as P

BLK = 128
LANES = 128
NEG = -1e30
MESH = pl.DeviceIdType.MESH


def flipped(me, code):
    out = me
    bit = 1
    while bit <= code:
        if code & bit:
            out = out + bit * (1 - 2 * ((me // bit) % 2))
        bit *= 2
    return out


def kernel(n, kv, group, ctx, q_hbm, k_hbm, v_hbm, old_hbm, len_hbm, cnt_hbm,
           att_ref, heavy_ref,
           q_all, k_all, v_all, old_all, len_s, cnt_s, prob, part_out, part_in, stat,
           q_dma, k_dma, v_dma, misc_dma, q_send, q_recv, p_send, p_recv, s_send, s_recv):
    me = lax.axis_index("seq")
    rows = kv * group
    blocks = ctx // BLK
    stat_rows = (n * rows) // LANES
    hd = q_all.shape[-1]
    scale = hd ** -0.5
    seqs = [flipped(me, c) for c in range(n)]

    barrier = pltpu.get_barrier_semaphore()
    for c in range(1, n):
        pl.semaphore_signal(barrier, inc=1, device_id={"seq": seqs[c]}, device_id_type=MESH)

    q_copy = pltpu.make_async_copy(q_hbm.at[0], q_all.at[0], q_dma)
    q_copy.start()
    len_copy = pltpu.make_async_copy(len_hbm, len_s, misc_dma.at[0])
    len_copy.start()
    cnt_copy = pltpu.make_async_copy(cnt_hbm, cnt_s, misc_dma.at[1])
    cnt_copy.start()
    k_copies = [pltpu.make_async_copy(k_hbm.at[seqs[c]], k_all.at[c], k_dma.at[c]) for c in range(n)]
    v_copies = [pltpu.make_async_copy(v_hbm.at[seqs[c]], v_all.at[c], v_dma.at[c]) for c in range(n)]
    for c in range(n):
        k_copies[c].start()
        v_copies[c].start()
    old_copy = pltpu.make_async_copy(old_hbm, old_all, misc_dma.at[2])
    old_copy.start()

    q_copy.wait()
    pl.semaphore_wait(barrier, n - 1)

    def to_peer(src, dst, send_sem, recv_sem, c):
        return pltpu.make_async_remote_copy(
            src_ref=src, dst_ref=dst, send_sem=send_sem, recv_sem=recv_sem,
            device_id={"seq": seqs[c]}, device_id_type=MESH)

    q_sends = [to_peer(q_all.at[0], q_all.at[c], q_send.at[c], q_recv.at[c], c) for c in range(1, n)]
    for copy in reversed(q_sends):
        copy.start()

    lane = lax.broadcasted_iota(jnp.int32, (group, LANES), 1)
    sub = lax.broadcasted_iota(jnp.int32, (group, LANES), 0)
    lane_pair = lane // group
    per_row = LANES // group
    tops = [jnp.zeros((group, LANES), jnp.float32) for _ in range(stat_rows)]
    totals = [jnp.zeros((group, LANES), jnp.float32) for _ in range(stat_rows)]

    len_copy.wait()
    cnt_copy.wait()
    p_sends = []
    half = max(n // 2, 1)
    steps = [list(range(0, 1)), list(range(1, half)), list(range(half, n))]
    for codes in steps:
        for c in codes:
            if c:
                q_sends[c - 1].wait_recv()
            k_copies[c].wait()
            v_copies[c].wait()
        raw = {}
        for c in codes:
            for g in range(kv):
                full = lax.dot_general(q_all[c], k_all[c, g], (((1,), (1,)), ((), ())),
                                       preferred_element_type=jnp.float32)
                raw[c, g] = full[g * group:(g + 1) * group] * scale
        tight = {}
        for c in codes:
            b = seqs[c]
            seen = len_s[b] - me * ctx
            limits = [jnp.minimum(cnt_s[k, b], seen - k * BLK) for k in range(blocks)]
            for g in range(kv):
                masked = jnp.concatenate(
                    [jnp.where(lane < limits[k], raw[c, g][:, k * BLK:(k + 1) * BLK], NEG)
                     for k in range(blocks)], axis=1)
                top = jnp.max(masked, axis=1, keepdims=True)
                p = jnp.exp(masked - top)
                prob[c, g] = p
                total = jnp.sum(p, axis=1, keepdims=True)
                tight[c, g] = p
                pair = b * kv + g
                for r in range(stat_rows):
                    here = lane_pair == pair - r * per_row
                    tops[r] = jnp.where(here, top, tops[r])
                    totals[r] = jnp.where(here, total, totals[r])
        if codes is steps[-1]:
            diag = (lane % group) == sub
            for r in range(stat_rows):
                stat[0, r:r + 1, :] = jnp.sum(jnp.where(diag, tops[r], 0.0), axis=0, keepdims=True)
                stat[0, stat_rows + r:stat_rows + r + 1, :] = jnp.sum(
                    jnp.where(diag, totals[r], 0.0), axis=0, keepdims=True)
            s_sends = [to_peer(stat.at[0], stat.at[c], s_send.at[c], s_recv.at[c], c) for c in range(1, n)]
            for copy in reversed(s_sends):
                copy.start()
        for c in codes:
            wide = jnp.concatenate([tight[c, g] for g in range(kv)], axis=0).astype(jnp.bfloat16)
            mixed = jnp.concatenate(
                [jnp.dot(wide, v_all[c, g], preferred_element_type=jnp.float32)[g * group:(g + 1) * group]
                 for g in range(kv)], axis=0)
            if c:
                part_out[c] = mixed
            else:
                part_in[0] = mixed
        for c in reversed(codes):
            if c:
                copy = to_peer(part_out.at[c], part_in.at[c], p_send.at[c], p_recv.at[c], c)
                copy.start()
                p_sends.append(copy)

    old_copy.wait()
    for copy in s_sends:
        copy.wait_recv()

    fac = [[None] * stat_rows for _ in range(n)]
    for r in range(stat_rows):
        top_rows = [jnp.broadcast_to(stat[c, r:r + 1, :], (group, LANES)) for c in range(n)]
        tot_rows = [jnp.broadcast_to(stat[c, stat_rows + r:stat_rows + r + 1, :], (group, LANES)) for c in range(n)]
        best = functools.reduce(jnp.maximum, top_rows)
        scaled = [jnp.exp(t - best) for t in top_rows]
        whole = functools.reduce(jnp.add, [f * t for f, t in zip(scaled, tot_rows)])
        for c in range(n):
            fac[c][r] = scaled[c] / whole

    def column(row_list, pair):
        kept = [jnp.where(lane == pair * group - r * LANES + sub, row_list[r], 0.0)
                for r in range(stat_rows)]
        return jnp.sum(functools.reduce(jnp.add, kept), axis=1, keepdims=True)

    for c in range(n):
        b = seqs[c]
        for g in range(kv):
            share = column(fac[0], b * kv + g)
            add = jnp.sum(prob[c, g] * share, axis=0, keepdims=True)
            heavy_ref[b, g:g + 1, :] = old_all[b, g:g + 1, :] + add

    shares = [jnp.concatenate([column(fac[c], me * kv + g) for g in range(kv)], axis=0) for c in range(n)]
    for copy in p_sends:
        copy.wait_recv()
    att_ref[0] = functools.reduce(
        jnp.add, [shares[c] * part_in[c] for c in range(n)]).astype(jnp.bfloat16)
    for copy in q_sends + p_sends + s_sends:
        copy.wait_send()


def write_out(att_ref, heavy_ref, att_out, heavy_out, sems):
    copies = [pltpu.make_async_copy(att_ref, att_out, sems.at[0]),
              pltpu.make_async_copy(heavy_ref, heavy_out, sems.at[1])]
    for copy in copies:
        copy.start()
    for copy in copies:
        copy.wait()


def on_device(n, queries, keys, values, old_scores, lengths, valid_counts):
    own, rows, hd = queries.shape
    _, kv, ctx, _ = keys.shape
    group = rows // kv
    assert own == 1 and n & (n - 1) == 0 and (n * rows) % LANES == 0
    counts = valid_counts.T
    stat_rows = (n * rows) // LANES
    anywhere = pl.BlockSpec(memory_space=pl.ANY)
    vmem = pl.BlockSpec(memory_space=pltpu.VMEM)
    dma = pltpu.SemaphoreType.DMA
    att, heavy = pl.pallas_call(
        functools.partial(kernel, n, kv, group, ctx),
        out_shape=(pltpu.VMEM((own, rows, hd), jnp.bfloat16),
                   pltpu.VMEM(old_scores.shape, jnp.float32)),
        in_specs=[anywhere] * 6,
        out_specs=(vmem, vmem),
        scratch_shapes=[
            pltpu.VMEM((n, rows, hd), jnp.bfloat16),
            pltpu.VMEM((n, kv, ctx, hd), jnp.bfloat16),
            pltpu.VMEM((n, kv, ctx, hd), jnp.bfloat16),
            pltpu.VMEM(old_scores.shape, jnp.float32),
            pltpu.SMEM(lengths.shape, jnp.int32),
            pltpu.SMEM(counts.shape, jnp.int32),
            pltpu.VMEM((n, kv, group, ctx), jnp.float32),
            pltpu.VMEM((n, rows, hd), jnp.float32),
            pltpu.VMEM((n, rows, hd), jnp.float32),
            pltpu.VMEM((n, 2 * stat_rows, LANES), jnp.float32),
            dma, dma((n,)), dma((n,)), dma((3,)),
            dma((n,)), dma((n,)), dma((n,)), dma((n,)), dma((n,)), dma((n,)),
        ],
        compiler_params=pltpu.CompilerParams(collective_id=0, has_side_effects=True),
    )(queries, keys, values, old_scores, lengths, counts)
    return pl.pallas_call(
        write_out,
        out_shape=(jax.ShapeDtypeStruct(att.shape, att.dtype), jax.ShapeDtypeStruct(heavy.shape, heavy.dtype)),
        in_specs=[vmem, vmem],
        out_specs=(anywhere, anywhere),
        scratch_shapes=[dma((2,))],
        compiler_params=pltpu.CompilerParams(vmem_limit_bytes=2**20),
    )(att, heavy)


def solution(mesh):
    return jax.shard_map(
        functools.partial(on_device, mesh.shape["seq"]),
        mesh=mesh,
        in_specs=(
            P("seq", "head", None),
            P(None, "head", "seq", None),
            P(None, "head", "seq", None),
            P(None, "head", "seq"),
            P(),
            P(None, "seq"),
        ),
        out_specs=(P("seq", "head", None), P(None, "head", "seq")),
        check_vma=False,
    )
```

```python
import functools

import jax
import jax.numpy as jnp
from jax import lax
from jax.experimental import pallas as pl
from jax.experimental.pallas import tpu as pltpu
from jax.sharding import PartitionSpec as P

BLK = 128
LANES = 128
NEG = -1e30
MESH = pl.DeviceIdType.MESH


def flipped(me, code):
    out = me
    bit = 1
    while bit <= code:
        if code & bit:
            out = out + bit * (1 - 2 * ((me // bit) % 2))
        bit *= 2
    return out


def kernel(n, kv, group, ctx, q_hbm, k_hbm, v_hbm, old_hbm, len_hbm, cnt_hbm,
           att_ref, heavy_ref,
           q_all, k_all, v_all, old_all, len_s, cnt_s, prob, part_out, part_in, stat,
           q_dma, k_dma, v_dma, misc_dma, q_send, q_recv, p_send, p_recv, s_send, s_recv):
    me = lax.axis_index("seq")
    rows = kv * group
    blocks = ctx // BLK
    stat_rows = (n * rows) // LANES
    hd = q_all.shape[-1]
    scale = hd ** -0.5
    seqs = [flipped(me, c) for c in range(n)]

    barrier = pltpu.get_barrier_semaphore()
    for c in reversed(range(1, n)):
        pl.semaphore_signal(barrier, inc=1, device_id={"seq": seqs[c]}, device_id_type=MESH)

    q_copy = pltpu.make_async_copy(q_hbm.at[0], q_all.at[0], q_dma)
    q_copy.start()
    len_copy = pltpu.make_async_copy(len_hbm, len_s, misc_dma.at[0])
    len_copy.start()
    cnt_copy = pltpu.make_async_copy(cnt_hbm, cnt_s, misc_dma.at[1])
    cnt_copy.start()
    k_copies = [pltpu.make_async_copy(k_hbm.at[seqs[c]], k_all.at[c], k_dma.at[c]) for c in range(n)]
    v_copies = [pltpu.make_async_copy(v_hbm.at[seqs[c]], v_all.at[c], v_dma.at[c]) for c in range(n)]
    for c in range(n):
        k_copies[c].start()
        v_copies[c].start()
    old_copy = pltpu.make_async_copy(old_hbm, old_all, misc_dma.at[2])
    old_copy.start()

    q_copy.wait()
    pl.semaphore_wait(barrier, n - 1)

    def to_peer(src, dst, send_sem, recv_sem, c):
        return pltpu.make_async_remote_copy(
            src_ref=src, dst_ref=dst, send_sem=send_sem, recv_sem=recv_sem,
            device_id={"seq": seqs[c]}, device_id_type=MESH)

    q_sends = [to_peer(q_all.at[0], q_all.at[c], q_send.at[c], q_recv.at[c], c) for c in range(1, n)]
    for copy in reversed(q_sends):
        copy.start()

    lane = lax.broadcasted_iota(jnp.int32, (group, LANES), 1)
    sub = lax.broadcasted_iota(jnp.int32, (group, LANES), 0)
    lane_pair = lane // group
    per_row = LANES // group
    tops = [jnp.zeros((group, LANES), jnp.float32) for _ in range(stat_rows)]
    totals = [jnp.zeros((group, LANES), jnp.float32) for _ in range(stat_rows)]

    len_copy.wait()
    cnt_copy.wait()
    p_sends = []
    half = max(n // 2, 1)
    late = n - 1
    steps = [list(range(0, 1)), list(range(1, half)), list(range(half, late)), list(range(late, n))]
    for codes in steps:
        for c in codes:
            if c:
                q_sends[c - 1].wait_recv()
            k_copies[c].wait()
            v_copies[c].wait()
        raw = {}
        for c in codes:
            for g in range(kv):
                full = lax.dot_general(q_all[c], k_all[c, g], (((1,), (1,)), ((), ())),
                                       preferred_element_type=jnp.float32)
                raw[c, g] = full[g * group:(g + 1) * group] * scale
        tight = {}
        for c in codes:
            b = seqs[c]
            seen = len_s[b] - me * ctx
            limits = [jnp.minimum(cnt_s[k, b], seen - k * BLK) for k in range(blocks)]
            for g in range(kv):
                masked = jnp.concatenate(
                    [jnp.where(lane < limits[k], raw[c, g][:, k * BLK:(k + 1) * BLK], NEG)
                     for k in range(blocks)], axis=1)
                top = jnp.max(masked, axis=1, keepdims=True)
                p = jnp.exp(masked - top)
                prob[c, g] = p
                total = jnp.sum(p, axis=1, keepdims=True)
                tight[c, g] = p
                pair = b * kv + g
                for r in range(stat_rows):
                    here = lane_pair == pair - r * per_row
                    tops[r] = jnp.where(here, top, tops[r])
                    totals[r] = jnp.where(here, total, totals[r])
        if codes is steps[-1]:
            diag = (lane % group) == sub
            for r in range(stat_rows):
                stat[0, r:r + 1, :] = jnp.sum(jnp.where(diag, tops[r], 0.0), axis=0, keepdims=True)
                stat[0, stat_rows + r:stat_rows + r + 1, :] = jnp.sum(
                    jnp.where(diag, totals[r], 0.0), axis=0, keepdims=True)
            s_sends = [to_peer(stat.at[0], stat.at[c], s_send.at[c], s_recv.at[c], c) for c in range(1, n)]
            for copy in reversed(s_sends):
                copy.start()
        for c in codes:
            wide = jnp.concatenate([tight[c, g] for g in range(kv)], axis=0).astype(jnp.bfloat16)
            mixed = jnp.concatenate(
                [jnp.dot(wide, v_all[c, g], preferred_element_type=jnp.float32)[g * group:(g + 1) * group]
                 for g in range(kv)], axis=0)
            if c:
                part_out[c] = mixed
            else:
                part_in[0] = mixed
        for c in reversed(codes):
            if c:
                copy = to_peer(part_out.at[c], part_in.at[c], p_send.at[c], p_recv.at[c], c)
                copy.start()
                p_sends.append(copy)

    old_copy.wait()
    for copy in s_sends:
        copy.wait_recv()

    fac = [[None] * stat_rows for _ in range(n)]
    for r in range(stat_rows):
        top_rows = [jnp.broadcast_to(stat[c, r:r + 1, :], (group, LANES)) for c in range(n)]
        tot_rows = [jnp.broadcast_to(stat[c, stat_rows + r:stat_rows + r + 1, :], (group, LANES)) for c in range(n)]
        best = functools.reduce(jnp.maximum, top_rows)
        scaled = [jnp.exp(t - best) for t in top_rows]
        whole = functools.reduce(jnp.add, [f * t for f, t in zip(scaled, tot_rows)])
        for c in range(n):
            fac[c][r] = scaled[c] / whole

    def column(row_list, pair):
        kept = [jnp.where(lane == pair * group - r * LANES + sub, row_list[r], 0.0)
                for r in range(stat_rows)]
        return jnp.sum(functools.reduce(jnp.add, kept), axis=1, keepdims=True)

    for c in range(n):
        b = seqs[c]
        for g in range(kv):
            share = column(fac[0], b * kv + g)
            add = jnp.sum(prob[c, g] * share, axis=0, keepdims=True)
            heavy_ref[b, g:g + 1, :] = old_all[b, g:g + 1, :] + add

    shares = [jnp.concatenate([column(fac[c], me * kv + g) for g in range(kv)], axis=0) for c in range(n)]
    for copy in p_sends:
        copy.wait_recv()
    att_ref[0] = functools.reduce(
        jnp.add, [shares[c] * part_in[c] for c in range(n)]).astype(jnp.bfloat16)
    for copy in q_sends + p_sends + s_sends:
        copy.wait_send()


def write_out(att_ref, heavy_ref, att_out, heavy_out, sems):
    copies = [pltpu.make_async_copy(att_ref, att_out, sems.at[0]),
              pltpu.make_async_copy(heavy_ref, heavy_out, sems.at[1])]
    for copy in copies:
        copy.start()
    for copy in copies:
        copy.wait()


def on_device(n, queries, keys, values, old_scores, lengths, valid_counts):
    own, rows, hd = queries.shape
    _, kv, ctx, _ = keys.shape
    group = rows // kv
    assert own == 1 and n & (n - 1) == 0 and (n * rows) % LANES == 0
    counts = valid_counts.T
    stat_rows = (n * rows) // LANES
    anywhere = pl.BlockSpec(memory_space=pl.ANY)
    vmem = pl.BlockSpec(memory_space=pltpu.VMEM)
    dma = pltpu.SemaphoreType.DMA
    att, heavy = pl.pallas_call(
        functools.partial(kernel, n, kv, group, ctx),
        out_shape=(pltpu.VMEM((own, rows, hd), jnp.bfloat16),
                   pltpu.VMEM(old_scores.shape, jnp.float32)),
        in_specs=[anywhere] * 6,
        out_specs=(vmem, vmem),
        scratch_shapes=[
            pltpu.VMEM((n, rows, hd), jnp.bfloat16),
            pltpu.VMEM((n, kv, ctx, hd), jnp.bfloat16),
            pltpu.VMEM((n, kv, ctx, hd), jnp.bfloat16),
            pltpu.VMEM(old_scores.shape, jnp.float32),
            pltpu.SMEM(lengths.shape, jnp.int32),
            pltpu.SMEM(counts.shape, jnp.int32),
            pltpu.VMEM((n, kv, group, ctx), jnp.float32),
            pltpu.VMEM((n, rows, hd), jnp.float32),
            pltpu.VMEM((n, rows, hd), jnp.float32),
            pltpu.VMEM((n, 2 * stat_rows, LANES), jnp.float32),
            dma, dma((n,)), dma((n,)), dma((3,)),
            dma((n,)), dma((n,)), dma((n,)), dma((n,)), dma((n,)), dma((n,)),
        ],
        compiler_params=pltpu.CompilerParams(collective_id=0, has_side_effects=True),
    )(queries, keys, values, old_scores, lengths, counts)
    return pl.pallas_call(
        write_out,
        out_shape=(jax.ShapeDtypeStruct(att.shape, att.dtype), jax.ShapeDtypeStruct(heavy.shape, heavy.dtype)),
        in_specs=[vmem, vmem],
        out_specs=(anywhere, anywhere),
        scratch_shapes=[dma((2,))],
        compiler_params=pltpu.CompilerParams(vmem_limit_bytes=2**20),
    )(att, heavy)


def solution(mesh):
    return jax.shard_map(
        functools.partial(on_device, mesh.shape["seq"]),
        mesh=mesh,
        in_specs=(
            P("seq", "head", None),
            P(None, "head", "seq", None),
            P(None, "head", "seq", None),
            P(None, "head", "seq"),
            P(),
            P(None, "seq"),
        ),
        out_specs=(P("seq", "head", None), P(None, "head", "seq")),
        check_vma=False,
    )
```
